32 devices in a mesh: ep: 4 (over y, x), fsdp: 8 (over z, core).
Axes of the slice: x: 2, y: 2, z: 4, core: 2. Of those that a mesh axis runs over, the one named last changes fastest.
Arguments:
- train_gate: float32 [64, 2048, 1408], P('ep', 'fsdp'), may hold values from -0.1875 to 0.1875
- train_up: float32 [64, 2048, 1408], P('ep', 'fsdp'), may hold values from -0.1875 to 0.1875
- train_down: float32 [64, 1408, 2048], P('ep', None, 'fsdp'), may hold values from -0.21875 to 0.21875
- router_weight: float32 [2048, 64], P('fsdp', 'ep'), may hold values from -0.125 to 0.125
- router_gain: float32 [2048], P('fsdp'), may hold values from 0.25 to 1.75
Outputs:
- ready_gate: bfloat16 [64, 2048, 1408], P('ep', None, 'fsdp')
- ready_up: bfloat16 [64, 2048, 1408], P('ep', None, 'fsdp')
- ready_down: bfloat16 [64, 1408, 2048], P('ep', 'fsdp')
- scale_gate: float32 [64, 1408], P('ep', 'fsdp')
- scale_up: float32 [64, 1408], P('ep', 'fsdp')
- scale_down: float32 [64, 1408], P('ep', 'fsdp')
- serve_router: bfloat16 [2048, 64], replicated
The draws below stay inside these ranges and needn't reach their ends.
All inputs are finite; a program needn't handle non-finite values. Where the reference program divides by a largest or mean magnitude, that divisor is 1e-20 or more.
Results may differ from the reference program's by a relative error of at most 0.001.
Values may be sent and summed in bfloat16 or wider, within the bound.
A program may use at most 256 MiB of HBM per device.

```python
import jax
import jax.numpy as jnp

EXPERTS = 64
D_MODEL = 2048
D_EXPERT = 1408


def with_spikes(result, rng, source, target, shards_of, factor):
    def block_of(dim):
        return (jnp.arange(result.shape[dim]) // (result.shape[dim] // shards_of)).reshape((-1,) + (1,) * (result.ndim - 1 - dim))

    near = jax.random.permutation(rng, shards_of)[block_of(target)]
    other_side = (block_of(target) + shards_of // 2) % shards_of
    return jnp.where((block_of(source) == near) | (block_of(source) == other_side), factor * result, result)


def shard_levels(key, dims, pieces, low, largest):
    level, own = 1.0, jax.random.fold_in(key, 6)
    for position, shards_of in pieces:
        steps = jnp.exp(jax.random.uniform(jax.random.fold_in(own, position), (shards_of,), jnp.float32, low / len(pieces), largest / len(pieces)))
        level = level * jnp.repeat(steps, dims[position] // shards_of).reshape([-1 if axis == position else 1 for axis in range(len(dims))])
    return level


def centred(rng, shape, deviation, most, shards=(), kind=jnp.bfloat16):
    result = deviation * jax.random.normal(rng, shape, jnp.float32)
    if shards:
        result = result * shard_levels(rng, shape, shards, -0.22, 0.18)
    return jnp.clip(result, -most, most).astype(kind)


def bell_draw_with(own_key, shape, width, reach, shards, heavy, held_as=jnp.bfloat16):
    drawn = width * jax.random.normal(own_key, shape, jnp.float32)
    if shards:
        drawn = drawn * shard_levels(own_key, shape, shards, -0.22, 0.18)
    return jnp.clip(with_spikes(drawn, jax.random.fold_in(own_key, 3), *heavy), -reach, reach).astype(held_as)


def setup_inputs(seed: int = 0) -> dict:
    keys = jax.random.split(jax.random.key(seed), 6)
    train_gate = bell_draw_with(keys[0], (EXPERTS, D_MODEL, D_EXPERT), D_MODEL ** -0.5, 0.1875, ((0, 4), (1, 8)), (1, 2, 8, 2.0), jnp.float32)
    train_up = bell_draw_with(keys[1], (EXPERTS, D_MODEL, D_EXPERT), D_MODEL ** -0.5, 0.1875, ((0, 4), (1, 8)), (1, 2, 8, 2.0), jnp.float32)
    train_down = bell_draw_with(keys[2], (EXPERTS, D_EXPERT, D_MODEL), D_EXPERT ** -0.5, 0.21875, ((0, 4), (2, 8)), (2, 1, 8, 2.0), jnp.float32)
    router_weight = centred(keys[3], (D_MODEL, EXPERTS), D_MODEL ** -0.5, 0.125, ((0, 8), (1, 4)), jnp.float32)
    router_gain = jnp.clip(1.0 + 0.15 * jax.random.normal(keys[4], (D_MODEL,), jnp.float32), 0.25, 1.75)
    return {"train_gate": train_gate, "train_up": train_up, "train_down": train_down, "router_weight": router_weight, "router_gain": router_gain}


def reference(train_gate, train_up, train_down, router_weight, router_gain):
    scale_gate = jnp.max(jnp.abs(train_gate), axis=1)
    ready_gate = (train_gate / jnp.expand_dims(scale_gate, 1)).astype(jnp.bfloat16)
    scale_up = jnp.max(jnp.abs(train_up), axis=1)
    ready_up = (train_up / jnp.expand_dims(scale_up, 1)).astype(jnp.bfloat16)
    scale_down = jnp.max(jnp.abs(train_down), axis=2)
    ready_down = (train_down / jnp.expand_dims(scale_down, 2)).astype(jnp.bfloat16)
    serve_router = (router_weight * router_gain[:, None]).astype(jnp.bfloat16)
    return ready_gate, ready_up, ready_down, scale_gate, scale_up, scale_down, serve_router
```

```python
import jax
import jax.numpy as jnp
from jax import lax
from jax.sharding import PartitionSpec as P


def after(value, earlier):
    return lax.optimization_barrier((value, earlier))[0]


def per_device(train_gate, train_up, train_down, router_weight, router_gain):
    scale_gate, scale_up, scale_down = lax.pmax(
        (
            jnp.max(jnp.abs(train_gate), axis=1),
            jnp.max(jnp.abs(train_up), axis=1),
            jnp.max(jnp.abs(train_down), axis=2),
        ),
        "fsdp",
    )
    narrow_gate, narrow_up, narrow_down = (
        (train_gate / jnp.expand_dims(scale_gate, 1)).astype(jnp.bfloat16),
        (train_up / jnp.expand_dims(scale_up, 1)).astype(jnp.bfloat16),
        (train_down / jnp.expand_dims(scale_down, 2)).astype(jnp.bfloat16),
    )
    ready_gate, ready_up = (
        lax.all_to_all(narrow_gate, "fsdp", split_axis=2, concat_axis=1, tiled=True),
        lax.all_to_all(narrow_up, "fsdp", split_axis=2, concat_axis=1, tiled=True),
    )
    ready_down = lax.all_to_all(after(narrow_down, ready_gate), "fsdp", split_axis=1, concat_axis=2, tiled=True)
    scale_gate = lax.dynamic_slice_in_dim(
        scale_gate, lax.axis_index("fsdp") * ready_gate.shape[2], ready_gate.shape[2], axis=1
    )
    scale_up = lax.dynamic_slice_in_dim(
        scale_up, lax.axis_index("fsdp") * ready_up.shape[2], ready_up.shape[2], axis=1
    )
    scale_down = lax.dynamic_slice_in_dim(
        scale_down, lax.axis_index("fsdp") * ready_down.shape[1], ready_down.shape[1], axis=1
    )
    part_router = (router_weight * router_gain[:, None]).astype(jnp.bfloat16)
    wide_router = lax.all_gather(after(part_router, ready_up), "ep", axis=1, tiled=True)
    serve_router = lax.all_gather(wide_router, "fsdp", axis=0, tiled=True)
    return (ready_gate, ready_up, ready_down, scale_gate, scale_up, scale_down, serve_router)


def solution(mesh):
    placed = (
        P("ep", "fsdp", None),
        P("ep", "fsdp", None),
        P("ep", None, "fsdp"),
        P("fsdp", "ep"),
        P("fsdp"),
    )
    return jax.shard_map(
        per_device,
        mesh=mesh,
        in_specs=placed,
        out_specs=(
            P("ep", None, "fsdp"),
            P("ep", None, "fsdp"),
            P("ep", "fsdp", None),
            P("ep", "fsdp"),
            P("ep", "fsdp"),
            P("ep", "fsdp"),
            P(),
        ),
        check_vma=False,
    )
```
